32 devices in a mesh: dp: 4 (over y, x), tensor: 8 (over z, core).
Axes of the slice: x: 2, y: 2, z: 4, core: 2. Of those that a mesh axis runs over, the one named last changes fastest.
Arguments:
- tokens: bfloat16 [2048, 4096], P(('dp', 'tensor')), parts along dimension 0, may hold values from -6 to 6
- norm_gain: float32 [4096], replicated, may hold values from 0.5 to 1.5
- gate_weight: bfloat16 [4096, 14336], P(None, 'tensor'), may hold values from -0.09375 to 0.09375
- up_weight: bfloat16 [4096, 14336], P(None, 'tensor'), may hold values from -0.09375 to 0.09375
- down_weight: bfloat16 [14336, 4096], P('tensor'), may hold values from -0.0625 to 0.0625
Outputs:
- mixed: bfloat16 [2048, 4096], P('dp', 'tensor'), parts along dimension 0
The draws below stay inside these ranges and needn't reach their ends.
There are 4 independent parts, one for each index of `dp`. The reference program is written for one: setup_inputs(seed, part) draws one part's arguments, and reference() takes and returns one part's arrays. A program takes and returns all parts, laid end to end along the dimension named above; an argument that names none is the same for every part. Nothing has to cross between parts.
All inputs are finite; a program needn't handle non-finite values.
Results may differ from the reference program's by a relative error of at most 0.0053.
Values may be sent and summed in bfloat16 or wider, within the bound.
No kernel may reach another device: no remote copies, remote signals or barrier semaphores. Data moves between devices by JAX's collectives and lax.ppermute only.
A program may use at most 128 MiB of HBM per device.

```python
import jax
import jax.numpy as jnp
from jax import lax

D = 4096
FF = 14336
TOKENS = 512


def raised(entries, key, source, target, blocks, factor):
    owner, partner = [(jnp.arange(entries.shape[axis_at]) // (entries.shape[axis_at] // blocks)).reshape([-1 if axis == axis_at else 1 for axis in range(entries.ndim)]) for axis_at in (source, target)]
    chosen = jax.random.permutation(key, blocks)[partner]
    strong = (owner == chosen) | (owner == (partner + blocks // 2) % blocks)
    return jnp.where(strong, factor * entries, entries)


def levels(rng, extent, cuts, smallest, high):
    factor_of = 1.0
    for axis_at, parts in cuts:
        heights = jax.random.uniform(jax.random.fold_in(jax.random.fold_in(rng, 6), axis_at), (parts,), jnp.float32, smallest / len(cuts), high / len(cuts))
        factor_of = factor_of * jnp.repeat(jnp.exp(heights), extent[axis_at] // parts).reshape((-1,) + (1,) * (len(extent) - 1 - axis_at))
    return factor_of


def centred(stream_key, dims, spread, most, cuts=(), dtype=jnp.bfloat16):
    gain = levels(stream_key, dims, cuts, -0.22, 0.18) if cuts else 1.0
    drawn = jax.random.normal(stream_key, dims, jnp.float32) * spread * gain
    return jnp.minimum(jnp.maximum(drawn, -most), most).astype(dtype)


def bell_draw_with(rng, extent, spread, bound, shards, heavy, held_as=jnp.bfloat16):
    entries = spread * jax.random.normal(rng, extent, jnp.float32)
    if shards:
        entries = entries * levels(rng, extent, shards, -0.22, 0.18)
    return jnp.clip(raised(entries, jax.random.fold_in(rng, 3), *heavy), -bound, bound).astype(held_as)


def setup_inputs(seed: int = 0, part: int = 0) -> dict:
    streams_of = jax.random.split(jax.random.key(seed), 6)
    part_keys = jax.random.split(jax.random.fold_in(streams_of[5], part), 6)
    tokens = centred(part_keys[0], (TOKENS, D), 1.0, 6.0, ((0, 8),))
    norm_gain = jnp.clip(1.0 + 0.1 * jax.random.normal(streams_of[1], (D,), jnp.float32), 0.5, 1.5)
    gate_weight = centred(streams_of[2], (D, FF), D ** -0.5, 0.09375, ((1, 8),))
    up_weight = centred(streams_of[3], (D, FF), D ** -0.5, 0.09375, ((1, 8),))
    down_weight = bell_draw_with(streams_of[4], (FF, D), FF ** -0.5, 0.0625, ((0, 8),), (0, 1, 8, 2.0))
    return {"tokens": tokens, "norm_gain": norm_gain, "gate_weight": gate_weight, "up_weight": up_weight, "down_weight": down_weight}


def reference(tokens, norm_gain, gate_weight, up_weight, down_weight):
    wide = tokens.astype(jnp.float32)
    square_mean = lax.optimization_barrier(jnp.mean(wide * wide, axis=1, keepdims=True))
    normed = (wide * norm_gain[None, :] / jnp.sqrt(square_mean + 1e-05)).astype(jnp.bfloat16)
    gate = jnp.dot(normed, gate_weight, preferred_element_type=jnp.float32)
    up = jnp.dot(normed, up_weight, preferred_element_type=jnp.float32)
    hidden = (jax.nn.silu(gate) * up).astype(jnp.bfloat16)
    branch = jnp.dot(hidden, down_weight, preferred_element_type=jnp.float32)
    return (wide + branch).astype(jnp.bfloat16)
```

```python
import functools

import jax
import jax.numpy as jnp
from jax import lax
from jax.experimental import pallas as pl
from jax.experimental.pallas import tpu as pltpu
from jax.sharding import PartitionSpec as P


PARTS = 2


def tile_of(width):
    return next(t for t in (256, 128) if width % t == 0)


def ring_indices(n):
    return [2 * q + 1 if q < n // 2 else 2 * (n - 1 - q) for q in range(n)]


def up_kernel(n, rank, *refs):
    blocks, (gain, gate_weight, up_weight, hidden, residual, normed) = refs[:n], refs[n:]
    rows = blocks[0].shape[0]
    columns = residual.shape[1]

    @pl.when(pl.program_id(0) == 0)
    def _():
        mine = pl.multiple_of(rank[0] * columns, columns)
        for k in range(n):
            at = pl.ds(pl.multiple_of(rank[k] * rows, rows), rows)
            wide = blocks[k][...].astype(jnp.float32)
            square_mean = jnp.mean(wide * wide, axis=1, keepdims=True)
            scale = lax.rsqrt(square_mean + 1e-05)
            normed[at, :] = (wide * gain[...] * scale).astype(jnp.bfloat16)
            residual[at, :] = blocks[k][:, pl.ds(mine, columns)]

    gate = jnp.dot(normed[...], gate_weight[...], preferred_element_type=jnp.float32)
    up = jnp.dot(normed[...], up_weight[...], preferred_element_type=jnp.float32)
    hidden[...] = (gate / (1.0 + jnp.exp(-gate)) * up).astype(jnp.bfloat16)


def up_part(rank, blocks, gain, gate_weight, up_weight):
    n = len(blocks)
    rows, width = blocks[0].shape
    units = gate_weight.shape[1]
    tile = tile_of(units)
    columns = width // n
    whole = lambda i, rank: (0, 0)
    return pl.pallas_call(
        functools.partial(up_kernel, n),
        grid_spec=pltpu.PrefetchScalarGridSpec(
            num_scalar_prefetch=1,
            grid=(units // tile,),
            in_specs=[pl.BlockSpec((rows, width), whole)] * n
            + [
                pl.BlockSpec((1, width), whole),
                pl.BlockSpec((width, tile), lambda i, rank: (0, i)),
                pl.BlockSpec((width, tile), lambda i, rank: (0, i)),
            ],
            out_specs=[
                pl.BlockSpec((n * rows, tile), lambda i, rank: (0, i)),
                pl.BlockSpec((n * rows, columns), whole),
            ],
            scratch_shapes=[pltpu.VMEM((n * rows, width), jnp.bfloat16)],
        ),
        out_shape=[
            jax.ShapeDtypeStruct((n * rows, units), jnp.bfloat16),
            jax.ShapeDtypeStruct((n * rows, columns), jnp.bfloat16),
        ],
        compiler_params=pltpu.CompilerParams(dimension_semantics=("arbitrary",), vmem_limit_bytes=40 * 2**20),
        cost_estimate=pl.CostEstimate(
            flops=4 * n * rows * width * units, bytes_accessed=4 * width * units, transcendentals=n * rows * units
        ),
        name="up_part",
    )(rank, *blocks, gain, gate_weight, up_weight)


def down_kernel(order, rank, hidden, down_weight, *outs):
    product = jnp.dot(hidden[...], down_weight[...], preferred_element_type=jnp.float32)
    for i, k in enumerate(order):

        @pl.when(pl.program_id(0) == i)
        def _(k=k):
            outs[k][...] = product.astype(outs[k].dtype)


def down_part(rank, order, hidden, down_weight):
    n = len(order)
    rows, units = hidden.shape
    columns = down_weight.shape[1] // n

    def place(i, rank):
        k = order[-1]
        for j, other in enumerate(order[:-1]):
            k = jnp.where(i == j, other, k)
        return 0, rank[k]

    whole = lambda i, rank: (0, 0)
    sent = {n // 2, n // 2 - 1, n // 2 + 1}
    return pl.pallas_call(
        functools.partial(down_kernel, order),
        grid_spec=pltpu.PrefetchScalarGridSpec(
            num_scalar_prefetch=1,
            grid=(n,),
            in_specs=[pl.BlockSpec((rows, units), whole), pl.BlockSpec((units, columns), place)],
            out_specs=[pl.BlockSpec((rows, columns), whole)] * n,
        ),
        out_shape=[
            jax.ShapeDtypeStruct((rows, columns), jnp.bfloat16 if k == n // 2 else jnp.float32) for k in range(n)
        ],
        compiler_params=pltpu.CompilerParams(dimension_semantics=("arbitrary",), vmem_limit_bytes=40 * 2**20),
        cost_estimate=pl.CostEstimate(
            flops=2 * n * rows * units * columns, bytes_accessed=2 * n * units * columns, transcendentals=0
        ),
        name="down_part",
    )(rank, hidden, down_weight)


def on_device(tokens, norm_gain, gate_weight, up_weight, down_weight):
    n = lax.axis_size("tensor")
    half = n // 2
    reach = half - 1
    ring = ring_indices(n)
    clockwise = [(ring[q], ring[(q + 1) % n]) for q in range(n)]
    counter = [(b, a) for a, b in clockwise]
    pair = [(t, t ^ 1) for t in range(n)]

    me = lax.axis_index("tensor")
    place = jnp.where(me % 2 == 1, me // 2, n - 1 - me // 2)
    q = (place + jnp.arange(n, dtype=jnp.int32)) % n
    rank = jnp.where(q < half, 2 * q + 1, 2 * (n - 1 - q))
    lacks = (half - 1 - 2 * place) % n

    def send(value, links):
        return lax.ppermute(value, "tensor", links)

    def chosen(by_offset):
        odd = [k for k in range(1, n, 2)]
        value = by_offset[odd[0]]
        for k in odd[1:]:
            value = jnp.where(lacks == k, by_offset[k], value)
        return value

    rows = tokens.shape[0] // PARTS
    gain = norm_gain[None, :]
    order = [half] + [k for d in range(reach, 0, -1) for k in (d, n - d)] + [0]

    pieces = []
    for part in range(PARTS):
        own = tokens[part * rows : (part + 1) * rows]
        by_offset = {0: own}
        ahead = behind = own
        for d in range(1, reach + 1):
            behind, ahead = send(behind, clockwise), send(ahead, counter)
            by_offset[n - d], by_offset[d] = behind, ahead
        by_offset[half] = send(chosen(by_offset), pair)
        pieces.append([by_offset[k] for k in range(n)])

    finished = []
    for blocks in pieces:
        hidden, residual = up_part(rank, blocks, gain, gate_weight, up_weight)
        partial = down_part(rank, order, hidden, down_weight)
        handed = send(partial[half], pair)

        def own_part(k):
            if k % 2 == 0:
                return partial[k]
            return partial[k] + jnp.where(lacks == k, handed.astype(jnp.float32), 0.0)

        down_ring = up_ring = None
        for d in range(reach, 0, -1):
            forward, backward = own_part(d), own_part(n - d)
            if down_ring is not None:
                forward, backward = forward + down_ring.astype(jnp.float32), backward + up_ring.astype(jnp.float32)
            down_ring = send(forward.astype(jnp.bfloat16), clockwise)
            up_ring = send(backward.astype(jnp.bfloat16), counter)
        total = residual.astype(jnp.float32) + (
            partial[0] + down_ring.astype(jnp.float32) + up_ring.astype(jnp.float32)
        )
        finished.append(total.astype(jnp.bfloat16).reshape(n, rows, -1))
    return jnp.stack(finished, axis=1).reshape(n * PARTS * rows, -1)


def solution(mesh):
    return jax.shard_map(
        on_device,
        mesh=mesh,
        in_specs=(
            P(("dp", "tensor"), None),
            P(),
            P(None, "tensor"),
            P(None, "tensor"),
            P("tensor", None),
        ),
        out_specs=P("dp", "tensor"),
        check_vma=False,
    )
```
